256 devices in a mesh: rows: 256 (over z, y, x, core).
Axes of the slice: x: 4, y: 4, z: 8, core: 2. Of those that a mesh axis runs over, the one named last changes fastest.
Arguments:
- factor_b: float32 [131072, 512], P('rows'), may hold values from -6 to 6
- band_vals: float32 [64, 131072], P(None, 'rows'), may hold values from -0.3125 to 0.3125
- offsets: int32 [64], replicated, may hold values from -64 to 64, as said below
- sketch: float32 [1024, 512], replicated, may hold values from -0.1875 to 0.1875
Outputs:
- factor_z: float32 [131072, 512], P('rows')
The draws below stay inside these ranges and needn't reach their ends.
Inputs may be any that keep to these rules, and one draw needn't show every extreme that they name: 64 distinct offsets; -64 and 64 are always among them.
All inputs are finite; a program needn't handle non-finite values.
Results may differ from the reference program's by a relative error of at most 0.0035.
Values sent between devices are 32-bit elements; how exact they have to be, the bound alone decides.
No kernel may reach another device: no remote copies, remote signals or barrier semaphores. Data moves between devices by JAX's collectives and lax.ppermute only.
A program may use at most 64 MiB of HBM per device.

```python
import jax
import jax.numpy as jnp
from jax import lax

R = 512
HALF = 64
K = 64
ITERS = 2
ORDER = 131072


def draw_offsets(key, part):
    inner = jax.random.permutation(key, 2 * HALF - 1)[:K - 2] - (HALF - 1)
    edges = jnp.array([-HALF, HALF], dtype=jnp.int32)
    return jnp.concatenate([edges, inner.astype(jnp.int32)]).astype(jnp.int32)


def steps_of(rng, dims, shards, least, top_value):
    def one(axis_at, blocks):
        heights = jax.random.uniform(jax.random.fold_in(jax.random.fold_in(rng, 6), axis_at), (blocks,), jnp.float32, least / len(shards), top_value / len(shards))
        return jnp.repeat(jnp.exp(heights), dims[axis_at] // blocks).reshape((-1,) + (1,) * (len(dims) - axis_at - 1))

    gain = one(*shards[0])
    for cut in shards[1:]:
        gain = gain * one(*cut)
    return gain


def centred(rng, extent, width, reach, split=(), held_as=jnp.bfloat16):
    result = width * jax.random.normal(rng, extent, jnp.float32)
    if split:
        result = result * steps_of(rng, extent, split, -0.22, 0.18)
    return jnp.clip(result, -reach, reach).astype(held_as)


def setup_inputs(seed: int = 0) -> dict:
    seeds = jax.random.split(jax.random.key(seed), 5)
    return {
        "factor_b": centred(seeds[0], (ORDER, R), 1.0, 6.0, ((0, 256),), jnp.float32),
        "band_vals": centred(seeds[1], (K, ORDER), (6 * K) ** -0.5, 0.3125, ((1, 256),), jnp.float32),
        "offsets": draw_offsets(jax.random.fold_in(seeds[4], 71), 0),
        "sketch": centred(seeds[3], (2 * R, R), (2 * R) ** -0.5, 0.1875, (), jnp.float32),
    }


HIGH = lax.Precision.HIGHEST

def build_table(offsets, rim_width):
    block_rows = 2 * rim_width
    shape = (offsets.shape[0], block_rows, 2 * block_rows)
    row_ids = lax.broadcasted_iota(jnp.int32, shape, 1)
    col_ids = lax.broadcasted_iota(jnp.int32, shape, 2)
    return (col_ids == row_ids + rim_width + offsets.astype(jnp.int32)[:, None, None]).astype(jnp.float32)

def band_apply(onehot_table, diag_vals, padded):
    block_rows = onehot_table.shape[1]
    row_count = diag_vals.shape[1]
    block_count = row_count // block_rows
    dense_blocks = jnp.einsum('jbi,jic->bic', diag_vals.reshape(diag_vals.shape[0], block_count, block_rows), onehot_table, precision=HIGH)
    row_blocks = padded.reshape(block_count + 1, block_rows, padded.shape[1])
    windowed = jnp.concatenate([row_blocks[:-1], row_blocks[1:]], axis=1)
    result_rows = jnp.einsum('bic,bcr->bir', dense_blocks, windowed, precision=HIGH)
    return result_rows.reshape(row_count, padded.shape[1])

def compress(joined, sketched):
    normal = jnp.einsum('ar,as->rs', sketched, sketched, precision=HIGH)
    chol_factor = jnp.linalg.cholesky(normal)
    basis_t = lax.linalg.triangular_solve(chol_factor, sketched.T, left_side=True, lower=True)
    return jnp.einsum('nk,rk->nr', joined, basis_t, precision=HIGH)

def reference(factor_b, band_vals, offsets, sketch):
    onehot_table = build_table(offsets, HALF)
    factor = factor_b
    for doubling in range(ITERS):
        powered = factor
        for repeat_idx in range(2 ** doubling):
            padded = jnp.pad(powered, ((HALF, HALF), (0, 0)))
            powered = band_apply(onehot_table, band_vals, padded)
        joined = jnp.concatenate([factor, powered], axis=1)
        projected = jnp.dot(joined, sketch, precision=HIGH)
        sketched = jnp.einsum('nk,nr->kr', joined, projected, precision=HIGH)
        factor = compress(joined, sketched)
    return factor
```

```python
import jax
import jax.numpy as jnp
from jax import lax
from jax.experimental import pallas as pl
from jax.experimental.pallas import tpu as pltpu
from jax.sharding import Mesh
from jax.sharding import PartitionSpec as P

HALF = 64
ITERS = 2
ROWS = ("z", "y", "x", "c")
F32 = jnp.float32
BF16 = jnp.bfloat16

HIGH = lax.Precision.HIGHEST


def padded_2(shard, sides, width):
    for axis, dim in sides:
        size, length = (lax.axis_size(axis), shard.shape[dim])
        up = [(i, (i + 1) % size) for i in range(size - 1)]
        down = [(j, i) for i, j in up]
        last = lax.slice_in_dim(shard, length - width, length, axis=dim)
        first = lax.slice_in_dim(shard, 0, width, axis=dim)
        before = lax.ppermute(last, axis, up)
        after = lax.ppermute(first, axis, down)
        shard = jnp.concatenate([before, shard, after], axis=dim)
    return shard


def build_table(offsets, rim_width):
    block_rows = 2 * rim_width
    shape = (offsets.shape[0], block_rows, 2 * block_rows)
    row_ids = lax.broadcasted_iota(jnp.int32, shape, 1)
    col_ids = lax.broadcasted_iota(jnp.int32, shape, 2)
    return (col_ids == row_ids + rim_width + offsets[:, None, None]).astype(jnp.float32)


def band_apply(onehot_table, diag_vals, padded):
    block_rows = onehot_table.shape[1]
    row_count = diag_vals.shape[1]
    block_count = row_count // block_rows
    dense_blocks = jnp.einsum(
        "jbi,jic->bic",
        diag_vals.reshape(diag_vals.shape[0], block_count, block_rows),
        onehot_table,
        precision=HIGH,
    )
    row_blocks = padded.reshape(block_count + 1, block_rows, padded.shape[1])
    windowed = jnp.concatenate([row_blocks[:-1], row_blocks[1:]], axis=1)
    result_rows = jnp.einsum("bic,bcr->bir", dense_blocks, windowed, precision=HIGH)
    return result_rows.reshape(row_count, padded.shape[1])


BLOCK = 128
PANEL = 16


def split3(x):
    h = x.astype(BF16)
    r = x - h.astype(F32)
    m = r.astype(BF16)
    return h, m, (r - m.astype(F32)).astype(BF16)


def mul(a, b):
    return jnp.dot(a, b, preferred_element_type=F32)


def exact_dot(a, b):
    ah, am, al = split3(a)
    bh, bm, bl = split3(b)
    hm = jnp.concatenate([ah, am], 1)
    low = mul(hm, jnp.concatenate([bm, bm], 0))
    low += mul(jnp.concatenate([al, ah], 1), jnp.concatenate([bh, bl], 0))
    return mul(hm, jnp.concatenate([bh, bh], 0)) + low


def factor_block(d_block):
    n = d_block.shape[0]
    count = n // PANEL
    row_ids = lax.broadcasted_iota(jnp.int32, (n, n), 0)
    eye = (row_ids == lax.broadcasted_iota(jnp.int32, (n, n), 1)).astype(F32)
    both = jnp.concatenate([d_block, eye], 1)
    panels = [both[PANEL * q : PANEL * (q + 1)] for q in range(count)]
    sub = lax.broadcasted_iota(jnp.int32, (PANEL, n), 0)
    inverse = []
    for p in range(count):
        a, b = panels[p][:, :n], panels[p][:, n:]
        at = PANEL * p
        cols = [jnp.broadcast_to(a[:, at + j : at + j + 1], (PANEL, n)) for j in range(PANEL)]
        w = jnp.zeros((PANEL, n), F32)
        for k in range(PANEL):
            m = cols[k]
            root = lax.rsqrt(m[k : k + 1])
            inv = root * root
            keep = sub == k
            w = jnp.where(keep, b[k : k + 1] * root, w)
            a = jnp.where(keep, a[k : k + 1] * inv, a - m * (a[k : k + 1] * inv))
            b = jnp.where(keep, b[k : k + 1] * inv, b - m * (b[k : k + 1] * inv))
            for j in range(k + 1, PANEL):
                c = cols[j][k : k + 1] * inv
                cols[j] = jnp.where(keep, c, cols[j] - m * c)
        inverse.append(w)
        if p + 1 < count:
            parts = [jnp.zeros((at, 2 * n), F32)] if p else []
            parts += [jnp.concatenate([a, b], 1), jnp.zeros((n - at - PANEL, 2 * n), F32)]
            left = jnp.concatenate([panels[q][:, :n] for q in range(p + 1, count)], 0)
            change = exact_dot(left, jnp.concatenate(parts, 0))
            for q in range(p + 1, count):
                i = PANEL * (q - p - 1)
                panels[q] = panels[q] - change[i : i + PANEL]
    return jnp.concatenate(inverse, 0)


def inverse_body(normal_ref, out_ref, work_ref, row_ref):
    n = BLOCK
    count = normal_ref.shape[0] // n
    work_ref[...] = normal_ref[...]
    lane = lax.broadcasted_iota(jnp.int32, (n, count * n), 1) // n

    def step(b, carry):
        at = pl.multiple_of(b * n, n)
        w = factor_block(work_ref[pl.ds(at, n), pl.ds(at, n)])
        row = exact_dot(w, work_ref[pl.ds(at, n), :])
        row = jnp.where(lane == b, jnp.concatenate([w] * count, 1), row)
        row_ref[...] = row
        out_ref[pl.ds(at, n), :] = jnp.where(lane <= b, row, 0.0)

        def trail(i, carry):
            to = pl.multiple_of(i * n, n)
            left = row_ref[:, pl.ds(to, n)].T
            kept = jnp.where(lane == b, 0.0, work_ref[pl.ds(to, n), :])
            work_ref[pl.ds(to, n), :] = kept - exact_dot(left, row_ref[...])
            return carry

        lax.fori_loop(b + 1, count, trail, 0)
        return carry

    lax.fori_loop(0, count, step, 0)


def chol_inverse(normal):
    size = normal.shape[0]
    return pl.pallas_call(
        inverse_body,
        out_shape=jax.ShapeDtypeStruct((size, size), F32),
        in_specs=[pl.BlockSpec(memory_space=pltpu.VMEM)],
        out_specs=pl.BlockSpec(memory_space=pltpu.VMEM),
        scratch_shapes=[pltpu.VMEM((size, size), F32), pltpu.VMEM((BLOCK, size), F32)],
    )(normal)


def swap_cores(x):
    return lax.ppermute(x, "c", [(0, 1), (1, 0)])


def sum_over_rows(mine, other):
    half = mine + swap_cores(other)
    plane = lax.axis_size("y") * lax.axis_size("x")
    rows, width = half.shape
    blocks = half.reshape(plane, rows // plane, width)
    part = lax.all_to_all(blocks, ("y", "x"), 0, 0, tiled=True).sum(0)
    size = lax.axis_size("z")
    step = 1
    while step < size:
        part = part + lax.ppermute(part, "z", [(i, i ^ step) for i in range(size)])
        step *= 2
    copies = jnp.broadcast_to(part[None], blocks.shape)
    own = lax.all_to_all(copies, ("y", "x"), 0, 0, tiled=True).reshape(rows, width)
    return own, swap_cores(own)


def compress(factor, powered, sketch):
    joined = jnp.concatenate([factor, powered], axis=1)
    projected = jnp.dot(joined, sketch, precision=HIGH)
    local_sketch = jnp.einsum("nk,nr->kr", joined, projected, precision=HIGH)
    half = local_sketch.shape[0] // 2
    core = lax.axis_index("c")
    mine = lax.dynamic_slice_in_dim(local_sketch, core * half, half, 0)
    other = lax.dynamic_slice_in_dim(local_sketch, (1 - core) * half, half, 0)
    own, rest = sum_over_rows(mine, other)
    normal = jnp.einsum("ar,as->rs", own, own, precision=HIGH)
    normal += jnp.einsum("ar,as->rs", rest, rest, precision=HIGH)
    inverse = chol_inverse(normal)
    top = jnp.where(core == 0, own, rest)
    low = jnp.where(core == 0, rest, own)
    reached = jnp.dot(factor, top, precision=HIGH) + jnp.dot(powered, low, precision=HIGH)
    return jnp.einsum("nk,rk->nr", reached, inverse, precision=HIGH)


def per_device(factor_b, band_vals, offsets, sketch):
    onehot_table = build_table(offsets, HALF)
    factor = factor_b
    for doubling in range(ITERS):
        repeats = 2**doubling
        powered = padded_2(factor, ((ROWS, 0),), repeats * HALF)
        if repeats > 1:
            wide_vals = padded_2(band_vals, ((ROWS, 1),), (repeats - 1) * HALF)
        for repeat_idx in range(repeats):
            extra_rows = (repeats - 1 - repeat_idx) * HALF
            if extra_rows > 0:
                part_vals = wide_vals
            else:
                part_vals = band_vals
            powered = band_apply(onehot_table, part_vals, powered)
        factor = compress(factor, powered, sketch)
    return factor


def solution(mesh):
    split = Mesh(mesh.devices.reshape(8, 4, 4, 2), ROWS)
    return jax.shard_map(
        per_device,
        mesh=split,
        in_specs=(P(ROWS, None), P(None, ROWS), P(), P()),
        out_specs=P(ROWS, None),
        check_vma=False,
    )
```

```python
import jax
import jax.numpy as jnp
from jax import lax
from jax.experimental import pallas as pl
from jax.experimental.pallas import tpu as pltpu
from jax.sharding import Mesh
from jax.sharding import PartitionSpec as P

HALF = 64
ROWS = ("z", "y", "x", "c")
F32 = jnp.float32
BF16 = jnp.bfloat16
BLOCK = 128
PANEL = 16
VMEM = pl.BlockSpec(memory_space=pltpu.VMEM)
SMEM = pl.BlockSpec(memory_space=pltpu.SMEM)


def split2(x):
    h = x.astype(BF16)
    return h, (x - h.astype(F32)).astype(BF16)


def split3(x):
    h = x.astype(BF16)
    r = x - h.astype(F32)
    m = r.astype(BF16)
    return h, m, (r - m.astype(F32)).astype(BF16)


def mul(a, b, dims=(1, 0)):
    return lax.dot_general(a, b, (((dims[0],), (dims[1],)), ((), ())), preferred_element_type=F32)


def near_dot(a, b, dims=(1, 0)):
    return mul(a[0], b[0], dims) + (mul(a[0], b[1], dims) + mul(a[1], b[0], dims))


def exact_dot(a, b):
    ah, am, al = split3(a)
    bh, bm, bl = split3(b)
    hm = jnp.concatenate([ah, am], 1)
    low = mul(hm, jnp.concatenate([bm, bm], 0))
    low += mul(jnp.concatenate([al, ah], 1), jnp.concatenate([bh, bl], 0))
    return mul(hm, jnp.concatenate([bh, bh], 0)) + low


def factor_block(d_block):
    n = d_block.shape[0]
    count = n // PANEL
    row_ids = lax.broadcasted_iota(jnp.int32, (n, n), 0)
    eye = (row_ids == lax.broadcasted_iota(jnp.int32, (n, n), 1)).astype(F32)
    both = jnp.concatenate([d_block, eye], 1)
    panels = [both[PANEL * q : PANEL * (q + 1)] for q in range(count)]
    sub = lax.broadcasted_iota(jnp.int32, (PANEL, n), 0)
    inverse = []
    for p in range(count):
        a, b = panels[p][:, :n], panels[p][:, n:]
        at = PANEL * p
        cols = [jnp.broadcast_to(a[:, at + j : at + j + 1], (PANEL, n)) for j in range(PANEL)]
        w = jnp.zeros((PANEL, n), F32)
        for k in range(PANEL):
            m = cols[k]
            root = lax.rsqrt(m[k : k + 1])
            inv = root * root
            keep = sub == k
            w = jnp.where(keep, b[k : k + 1] * root, w)
            a = jnp.where(keep, a[k : k + 1] * inv, a - m * (a[k : k + 1] * inv))
            b = jnp.where(keep, b[k : k + 1] * inv, b - m * (b[k : k + 1] * inv))
            for j in range(k + 1, PANEL):
                c = cols[j][k : k + 1] * inv
                cols[j] = jnp.where(keep, c, cols[j] - m * c)
        inverse.append(w)
        if p + 1 < count:
            parts = [jnp.zeros((at, 2 * n), F32)] if p else []
            parts += [jnp.concatenate([a, b], 1), jnp.zeros((n - at - PANEL, 2 * n), F32)]
            left = jnp.concatenate([panels[q][:, :n] for q in range(p + 1, count)], 0)
            change = exact_dot(left, jnp.concatenate(parts, 0))
            for q in range(p + 1, count):
                i = PANEL * (q - p - 1)
                panels[q] = panels[q] - change[i : i + PANEL]
    return jnp.concatenate(inverse, 0)


def invert_factor(work_ref, row_ref, inv_ref):
    n = BLOCK
    count = work_ref.shape[0] // n
    lane = lax.broadcasted_iota(jnp.int32, (n, count * n), 1) // n

    def step(b, carry):
        at = pl.multiple_of(b * n, n)
        w = factor_block(work_ref[pl.ds(at, n), pl.ds(at, n)])
        row = exact_dot(w, work_ref[pl.ds(at, n), :])
        row = jnp.where(lane == b, jnp.concatenate([w] * count, 1), row)
        row_ref[...] = row
        high, low = split2(jnp.where(lane <= b, row, 0.0))
        inv_ref[0, pl.ds(at, n), :] = high
        inv_ref[1, pl.ds(at, n), :] = low

        def trail(i, carry):
            to = pl.multiple_of(i * n, n)
            left = row_ref[:, pl.ds(to, n)].T
            kept = jnp.where(lane == b, 0.0, work_ref[pl.ds(to, n), :])
            work_ref[pl.ds(to, n), :] = kept - exact_dot(left, row_ref[...])
            return carry

        lax.fori_loop(b + 1, count, trail, 0)
        return carry

    lax.fori_loop(0, count, step, 0)


def normal_matrix(own, rest, work_ref):
    size = work_ref.shape[0]
    parts = [split3(own), split3(rest)]
    for at in range(0, size, BLOCK):
        total = jnp.zeros((BLOCK, size - at), F32)
        for i, j in ((1, 1), (2, 0), (0, 2), (1, 0), (0, 1), (0, 0)):
            for side in parts:
                total += mul(side[i][:, at : at + BLOCK], side[j][:, at:], (0, 0))
        if at:
            work_ref[at : at + BLOCK, :at] = jnp.zeros((BLOCK, at), F32)
        work_ref[at : at + BLOCK, at:] = total


def powers_body(core, off, up, mid, down, v_up, v_mid, v_down, sketch, mine, other, parts, dense, long_ref):
    n = BLOCK
    size = mid.shape[0]
    width = mid.shape[1]
    lanes = lax.broadcasted_iota(jnp.int32, (off.shape[0], 2 * n), 1)
    hot = (off[...] + HALF == lanes).astype(BF16)
    hot = jnp.concatenate([hot, hot], 0)
    blocks = size // n + 2
    for i in range(blocks):
        if i == 0:
            v = v_up[...]
        elif i == blocks - 1:
            v = v_down[...]
        else:
            v = v_mid[:, n * (i - 1) : n * i]
        spread = mul(jnp.concatenate(split2(v), 0), hot, (0, 0))
        spread = pltpu.roll(spread, 0, 1, stride=1, stride_axis=0)
        dense[0, i], dense[1, i] = split2(spread)
    reach = 3 * HALF
    for half, (a, b, c) in enumerate(zip(split2(up[...]), split2(mid[...]), split2(down[...]))):
        long_ref[half, 0, :reach] = a
        long_ref[half, 0, reach : reach + size] = b
        long_ref[half, 0, reach + size :] = c
        parts[half, 0] = b
        edge = jnp.zeros((HALF, width), BF16)
        for level in (1, 2):
            long_ref[half, level, :HALF] = edge
            long_ref[half, level, size + 2 * reach - HALF :] = edge
    for level in range(3):
        for i in range(blocks) if level < 2 else range(1, blocks - 1):
            window = [long_ref[half, level, n * i : n * i + 2 * n] for half in range(2)]
            result = split2(near_dot((dense[0, i], dense[1, i]), window))
            for half in range(2):
                if level < 2:
                    long_ref[half, level + 1, n * i + HALF : n * i + HALF + n] = result[half]
                if 0 < i < blocks - 1:
                    parts[half, level + 1, n * (i - 1) : n * i] = result[half]
    gram_halves(core, parts, sketch, mine, other)


def gram_halves(core, parts, sketch, mine, other):
    size = parts.shape[2]
    top, low = (split2(sketch[size * s : size * (s + 1)]) for s in range(2))
    get = lambda s: (parts[0, s], parts[1, s])
    projected = split2(near_dot(get(0), top) + near_dot(get(1), low))
    c = core[0]
    mine[...] = near_dot(get(c), projected, (0, 0))
    other[...] = near_dot(get(1 - c), projected, (0, 0))


def next_body(core, own, rest, sketch, parts, mine, other, new_parts, work, row, inv):
    c = core[0]
    normal_matrix(own[...], rest[...], work)
    invert_factor(work, row, inv)
    sides = (split2(own[...]), split2(rest[...]))
    for s in range(2):
        reached = near_dot((parts[0, 2 * s + c], parts[1, 2 * s + c]), sides[0])
        reached += near_dot((parts[0, 2 * s + 1 - c], parts[1, 2 * s + 1 - c]), sides[1])
        result = near_dot(split2(reached), (inv[0], inv[1]), (1, 1))
        new_parts[0, s], new_parts[1, s] = split2(result)
    gram_halves(core, new_parts, sketch, mine, other)


def last_body(core, own, rest, parts, out, work, row, inv):
    c = core[0]
    normal_matrix(own[...], rest[...], work)
    invert_factor(work, row, inv)
    reached = near_dot((parts[0, c], parts[1, c]), split2(own[...]))
    reached += near_dot((parts[0, 1 - c], parts[1, 1 - c]), split2(rest[...]))
    out[...] = near_dot(split2(reached), (inv[0], inv[1]), (1, 1))


def shaped(*shape, dtype=F32):
    return jax.ShapeDtypeStruct(shape, dtype)


def inverse_scratch(width):
    return [
        pltpu.VMEM((width, width), F32),
        pltpu.VMEM((BLOCK, width), F32),
        pltpu.VMEM((2, width, width), BF16),
    ]


def powers(core, off, up, mid, down, v_up, v_mid, v_down, sketch):
    size, width = mid.shape
    return pl.pallas_call(
        powers_body,
        out_shape=(shaped(width, width), shaped(width, width), shaped(2, 4, size, width, dtype=BF16)),
        in_specs=[SMEM] + [VMEM] * 8,
        out_specs=(VMEM,) * 3,
        scratch_shapes=[
            pltpu.VMEM((2, size // BLOCK + 2, BLOCK, 2 * BLOCK), BF16),
            pltpu.VMEM((2, 3, size + 6 * HALF, width), BF16),
        ],
        name="powers",
    )(core, off, up, mid, down, v_up, v_mid, v_down, sketch)


def next_level(core, own, rest, sketch, parts):
    size, width = parts.shape[2:]
    return pl.pallas_call(
        next_body,
        out_shape=(shaped(width, width), shaped(width, width), shaped(2, 2, size, width, dtype=BF16)),
        in_specs=[SMEM] + [VMEM] * 4,
        out_specs=(VMEM,) * 3,
        scratch_shapes=inverse_scratch(width),
        name="next_level",
    )(core, own, rest, sketch, parts)


def last_level(core, own, rest, parts):
    size, width = parts.shape[2:]
    return pl.pallas_call(
        last_body,
        out_shape=shaped(size, width),
        in_specs=[SMEM] + [VMEM] * 3,
        out_specs=VMEM,
        scratch_shapes=inverse_scratch(width),
        name="last_level",
    )(core, own, rest, parts)


def swap_cores(x):
    return lax.ppermute(x, "c", [(0, 1), (1, 0)])


def sum_over_rows(mine, other):
    half = mine + swap_cores(other)
    plane = lax.axis_size("y") * lax.axis_size("x")
    rows, width = half.shape
    blocks = half.reshape(plane, rows // plane, width)
    part = lax.all_to_all(blocks, ("y", "x"), 0, 0, tiled=True).sum(0)
    size = lax.axis_size("z")
    for pairs in (
        [(i, i ^ 1) for i in range(size)],
        [(i, i ^ 2) for i in range(size)],
        [(i, size - 1 - i) for i in range(size)],
    ):
        part = part + lax.ppermute(part, "z", pairs)
    copies = jnp.broadcast_to(part[None], blocks.shape)
    own = lax.all_to_all(copies, ("y", "x"), 0, 0, tiled=True).reshape(rows, width)
    return own, swap_cores(own)


def from_neighbours(shard, dim, width):
    size, length = (lax.axis_size(ROWS), shard.shape[dim])
    up = [(i, i + 1) for i in range(size - 1)]
    down = [(j, i) for i, j in up]
    last = lax.slice_in_dim(shard, length - width, length, axis=dim)
    first = lax.slice_in_dim(shard, 0, width, axis=dim)
    return lax.ppermute(last, ROWS, up), lax.ppermute(first, ROWS, down)


def per_device(factor_b, band_vals, offsets, sketch):
    core = lax.axis_index("c").reshape(1)
    up, down = from_neighbours(factor_b, 0, 3 * HALF)
    v_up, v_down = from_neighbours(band_vals, 1, 2 * HALF)
    mine, other, parts = powers(
        core, offsets.reshape(-1, 1), up, factor_b, down, v_up, band_vals, v_down, sketch
    )
    own, rest = sum_over_rows(mine, other)
    mine, other, parts = next_level(core, own, rest, sketch, parts)
    own, rest = sum_over_rows(mine, other)
    return last_level(core, own, rest, parts)


def solution(mesh):
    split = Mesh(mesh.devices.reshape(8, 4, 4, 2), ROWS)
    return jax.shard_map(
        per_device,
        mesh=split,
        in_specs=(P(ROWS, None), P(None, ROWS), P(), P()),
        out_specs=P(ROWS, None),
        check_vma=False,
    )
```

```python
import jax
import jax.numpy as jnp
from jax import lax
from jax.experimental import pallas as pl
from jax.experimental.pallas import tpu as pltpu
from jax.sharding import Mesh
from jax.sharding import PartitionSpec as P

HALF = 64
ROWS = ("z", "y", "x", "c")
F32 = jnp.float32
BF16 = jnp.bfloat16
BLOCK = 128
PANEL = 16
VMEM = pl.BlockSpec(memory_space=pltpu.VMEM)
SMEM = pl.BlockSpec(memory_space=pltpu.SMEM)
PARAMS = pltpu.CompilerParams(vmem_limit_bytes=30 * 2**20)


def split2(x):
    h = x.astype(BF16)
    return h, (x - h.astype(F32)).astype(BF16)


def split3(x):
    h = x.astype(BF16)
    r = x - h.astype(F32)
    m = r.astype(BF16)
    return h, m, (r - m.astype(F32)).astype(BF16)


def mul(a, b, dims=(1, 0)):
    return lax.dot_general(a, b, (((dims[0],), (dims[1],)), ((), ())), preferred_element_type=F32)


def near_dot(a, b, dims=(1, 0)):
    return mul(a[0], b[0], dims) + (mul(a[0], b[1], dims) + mul(a[1], b[0], dims))


def exact_dot(a, b):
    ah, am, al = split3(a)
    bh, bm, bl = split3(b)
    hm = jnp.concatenate([ah, am], 1)
    low = mul(hm, jnp.concatenate([bm, bm], 0))
    low += mul(jnp.concatenate([al, ah], 1), jnp.concatenate([bh, bl], 0))
    return mul(hm, jnp.concatenate([bh, bh], 0)) + low


def factor_block(d_block):
    n = d_block.shape[0]
    count = n // PANEL
    rows = [d_block[i : i + 8] for i in range(0, n, 8)]
    sub = lax.broadcasted_iota(jnp.int32, (8, n), 0)
    lane = lax.broadcasted_iota(jnp.int32, (8, n), 1)
    spread = lambda x, r: jnp.broadcast_to(x[r % 8 : r % 8 + 1], (8, n))
    lanes = lambda x, at: jnp.broadcast_to(x[:, at : at + 1], (8, n))
    both = range(2)
    inverse = []
    for p in range(count):
        at = PANEL * p
        ours = (lane >= at) & (lane < at + PANEL)
        a = rows[2 * p : 2 * p + 2]
        cols = [[lanes(a[h], at + j) for h in both] for j in range(PANEL)]
        if p + 1 < count:
            below = [[lanes(rows[2 * p + 2 + h], at + j) for h in both] for j in range(PANEL)]
        left = rows[2 * p + 4 :]
        a = [jnp.where(ours, (lane == sub + (at + 8 * h)).astype(F32), a[h]) for h in both]
        w = [jnp.zeros((8, n), F32)] * 2
        scale = [jnp.zeros((8, n), F32)] * 2
        d = spread(cols[0][0], 0)
        for k in range(PANEL):
            g = k // 8
            here = sub == k % 8
            root = lax.rsqrt(d)
            inv = root * root
            m = list(cols[k])
            if k + 1 < PANEL:
                e = (k + 1) // 8
                cross = spread(m[e], k + 1) * spread(cols[k + 1][g], k)
                d = spread(cols[k + 1][e], k + 1) - cross * inv
            m[g] = jnp.where(here, 0.0, m[g])
            m = [m[h] * inv for h in both]
            row = spread(a[g], k)
            w[g] = jnp.where(here, row * root, w[g])
            scale[g] = jnp.where(here, inv, scale[g])
            a = [a[h] - m[h] * row for h in both]
            for j in range(k + 1, PANEL):
                c = spread(cols[j][g], k)
                cols[j] = [cols[j][h] - m[h] * c for h in both]
        inverse += w
        if p + 1 < count:
            a = [a[h] * scale[h] for h in both]
            wide = [spread(a[j // 8], j) for j in range(PANEL)]
            for h in both:
                r = 2 * p + 2 + h
                terms = [below[j][h] * wide[j] for j in range(PANEL)]
                while len(terms) > 1:
                    terms = [x + y for x, y in zip(terms[::2], terms[1::2])]
                rows[r] = jnp.where(ours, 0.0, rows[r]) - terms[0]
        if p + 2 < count:
            parts = ([jnp.zeros((at, n), F32)] if p else []) + a + [jnp.zeros((n - at - PANEL, n), F32)]
            change = exact_dot(jnp.concatenate(left, 0), jnp.concatenate(parts, 0))
            for i, r in enumerate(range(2 * p + 4, n // 8)):
                rows[r] = jnp.where(ours, 0.0, rows[r]) - change[8 * i : 8 * i + 8]
    inverse = jnp.concatenate(inverse, 0)
    row_ids = lax.broadcasted_iota(jnp.int32, (n, n), 0)
    return jnp.where(lax.broadcasted_iota(jnp.int32, (n, n), 1) <= row_ids, inverse, 0.0)


def invert_factor(work_ref, row_ref, inv_ref):
    n = BLOCK
    count = work_ref.shape[0] // n
    lane = lax.broadcasted_iota(jnp.int32, (n, count * n), 1) // n

    def step(b, carry):
        at = pl.multiple_of(b * n, n)
        w = factor_block(work_ref[pl.ds(at, n), pl.ds(at, n)])
        row = exact_dot(w, work_ref[pl.ds(at, n), :])
        row = jnp.where(lane == b, jnp.concatenate([w] * count, 1), row)
        row_ref[...] = row
        high, low = split2(jnp.where(lane <= b, row, 0.0))
        inv_ref[0, pl.ds(at, n), :] = high
        inv_ref[1, pl.ds(at, n), :] = low

        def trail(i, carry):
            to = pl.multiple_of(i * n, n)
            left = row_ref[:, pl.ds(to, n)].T
            kept = jnp.where(lane == b, 0.0, work_ref[pl.ds(to, n), :])
            work_ref[pl.ds(to, n), :] = kept - exact_dot(left, row_ref[...])
            return carry

        lax.fori_loop(b + 1, count, trail, 0)
        return carry

    lax.fori_loop(0, count, step, 0)


def normal_matrix(own, rest, work_ref):
    size = work_ref.shape[0]
    parts = [split3(own), split3(rest)]
    for at in range(0, size, BLOCK):
        total = jnp.zeros((BLOCK, size - at), F32)
        for i, j in ((1, 1), (2, 0), (0, 2), (1, 0), (0, 1), (0, 0)):
            for side in parts:
                total += mul(side[i][:, at : at + BLOCK], side[j][:, at:], (0, 0))
        if at:
            work_ref[at : at + BLOCK, :at] = jnp.zeros((BLOCK, at), F32)
        work_ref[at : at + BLOCK, at:] = total


def powers_body(core, off, near, far, mid, v_mid, sketch, mine, other, parts, dense, long_ref):
    n = BLOCK
    size = mid.shape[0]
    width = mid.shape[1]
    reach = 3 * HALF
    blocks = size // n + 2
    c = core[0]
    sides = ((near, 1 - c), (far, c))
    sub = lax.broadcasted_iota(jnp.int32, (8, 2 * n), 0)
    lanes = lax.broadcasted_iota(jnp.int32, (8, 2 * n), 1)
    hot = []
    for g in range(0, off.shape[0], 8):
        at = jnp.zeros((8, 2 * n), jnp.int32)
        for r in range(8):
            at = jnp.where(sub == r, off[g + r], at)
        hot.append((at + HALF == lanes).astype(F32))
    hot = jnp.concatenate(hot, 0).astype(BF16)
    hot = jnp.concatenate([hot, hot], 0)

    def spread(v, i):
        block = mul(jnp.concatenate(split2(v), 0), hot, (0, 0))
        block = pltpu.roll(block, 0, 1, stride=1, stride_axis=0)
        dense[0, i], dense[1, i] = split2(block)

    for i in range(1, blocks - 1):
        spread(v_mid[:, n * (i - 1) : n * i], i)
    for half, b in enumerate(split2(mid[...])):
        long_ref[half, 0, reach : reach + size] = b
        parts[half, 0] = b
        edge = jnp.zeros((HALF, width), BF16)
        for level in (1, 2):
            long_ref[half, level, :HALF] = edge
            long_ref[half, level, size + 2 * reach - HALF :] = edge
    for side, below in sides:
        at = pl.multiple_of(below * (reach + size), HALF)
        for i in range(width // n):
            for half, b in enumerate(split2(side[reach * i : reach * (i + 1)])):
                long_ref[half, 0, pl.ds(at, reach), n * i : n * (i + 1)] = b
        spread(side[reach * (width // n) :], below * (blocks - 1))
    for level in range(3):
        for i in range(blocks) if level < 2 else range(1, blocks - 1):
            window = [long_ref[half, level, n * i : n * i + 2 * n] for half in range(2)]
            result = split2(near_dot((dense[0, i], dense[1, i]), window))
            for half in range(2):
                if level < 2:
                    long_ref[half, level + 1, n * i + HALF : n * i + HALF + n] = result[half]
                if 0 < i < blocks - 1:
                    parts[half, level + 1, n * (i - 1) : n * i] = result[half]
    gram_halves(core, parts, sketch, mine, other)


def gram_halves(core, parts, sketch, mine, other):
    size = parts.shape[2]
    top, low = (split2(sketch[size * s : size * (s + 1)]) for s in range(2))
    get = lambda s: (parts[0, s], parts[1, s])
    projected = split2(near_dot(get(0), top) + near_dot(get(1), low))
    c = core[0]
    mine[...] = near_dot(get(c), projected, (0, 0))
    other[...] = near_dot(get(1 - c), projected, (0, 0))


def next_body(core, own, rest, sketch, parts, mine, other, new_parts, work, row, inv):
    c = core[0]
    normal_matrix(own[...], rest[...], work)
    invert_factor(work, row, inv)
    sides = (split2(own[...]), split2(rest[...]))
    for s in range(2):
        reached = near_dot((parts[0, 2 * s + c], parts[1, 2 * s + c]), sides[0])
        reached += near_dot((parts[0, 2 * s + 1 - c], parts[1, 2 * s + 1 - c]), sides[1])
        result = near_dot(split2(reached), (inv[0], inv[1]), (1, 1))
        new_parts[0, s], new_parts[1, s] = split2(result)
    gram_halves(core, new_parts, sketch, mine, other)


def last_body(core, own, rest, parts, out, work, row, inv):
    c = core[0]
    normal_matrix(own[...], rest[...], work)
    invert_factor(work, row, inv)
    reached = near_dot((parts[0, c], parts[1, c]), split2(own[...]))
    reached += near_dot((parts[0, 1 - c], parts[1, 1 - c]), split2(rest[...]))
    out[...] = near_dot(split2(reached), (inv[0], inv[1]), (1, 1))


def shaped(*shape, dtype=F32):
    return jax.ShapeDtypeStruct(shape, dtype)


def inverse_scratch(width):
    return [
        pltpu.VMEM((width, width), F32),
        pltpu.VMEM((BLOCK, width), F32),
        pltpu.VMEM((2, width, width), BF16),
    ]


def powers(core, off, near, far, mid, v_mid, sketch):
    size, width = mid.shape
    return pl.pallas_call(
        powers_body,
        out_shape=(shaped(width, width), shaped(width, width), shaped(2, 4, size, width, dtype=BF16)),
        in_specs=[SMEM] * 2 + [VMEM] * 5,
        out_specs=(VMEM,) * 3,
        scratch_shapes=[
            pltpu.VMEM((2, size // BLOCK + 2, BLOCK, 2 * BLOCK), BF16),
            pltpu.VMEM((2, 3, size + 6 * HALF, width), BF16),
        ],
        compiler_params=PARAMS,
        name="powers",
    )(core, off, near, far, mid, v_mid, sketch)


def next_level(core, own, rest, sketch, parts):
    size, width = parts.shape[2:]
    return pl.pallas_call(
        next_body,
        out_shape=(shaped(width, width), shaped(width, width), shaped(2, 2, size, width, dtype=BF16)),
        in_specs=[SMEM] + [VMEM] * 4,
        out_specs=(VMEM,) * 3,
        scratch_shapes=inverse_scratch(width),
        compiler_params=PARAMS,
        name="next_level",
    )(core, own, rest, sketch, parts)


def last_level(core, own, rest, parts):
    size, width = parts.shape[2:]
    return pl.pallas_call(
        last_body,
        out_shape=shaped(size, width),
        in_specs=[SMEM] + [VMEM] * 3,
        out_specs=VMEM,
        scratch_shapes=inverse_scratch(width),
        compiler_params=PARAMS,
        name="last_level",
    )(core, own, rest, parts)


def swap_cores(x):
    return lax.ppermute(x, "c", [(0, 1), (1, 0)])


def sum_over_rows(mine, other):
    half = mine + swap_cores(other)
    plane = lax.axis_size("y") * lax.axis_size("x")
    rows, width = half.shape
    blocks = half.reshape(plane, rows // plane, width)
    part = lax.all_to_all(blocks, ("y", "x"), 0, 0, tiled=True).sum(0)
    size = lax.axis_size("z")
    for pairs in (
        [(i, i ^ 1) for i in range(size)],
        [(i, i ^ 2) for i in range(size)],
        [(i, size - 1 - i) for i in range(size)],
    ):
        part = part + lax.ppermute(part, "z", pairs)
    copies = jnp.broadcast_to(part[None], blocks.shape)
    own = lax.all_to_all(copies, ("y", "x"), 0, 0, tiled=True).reshape(rows, width)
    return own, swap_cores(own)


def from_neighbours(factor, vals):
    core = lax.axis_index("c")
    reach, edge = 3 * HALF, 2 * HALF

    def packed(high):
        rows = lax.dynamic_slice_in_dim(factor, high * (factor.shape[0] - reach), reach, 0)
        cols = lax.dynamic_slice_in_dim(vals, high * (vals.shape[1] - edge), edge, 1)
        return jnp.concatenate([*jnp.split(rows, rows.shape[1] // edge, 1), cols], 0)

    size = lax.axis_size(ROWS)
    pairs = [(i, i + 1) for i in range(1, size - 1, 2)]
    pairs += [(j, i) for i, j in pairs]
    far = lax.ppermute(packed(core), ROWS, pairs)
    return swap_cores(packed(1 - core)), far


def per_device(factor_b, band_vals, offsets, sketch):
    core = lax.axis_index("c").reshape(1)
    near, far = from_neighbours(factor_b, band_vals)
    mine, other, parts = powers(core, offsets, near, far, factor_b, band_vals, sketch)
    own, rest = sum_over_rows(mine, other)
    mine, other, parts = next_level(core, own, rest, sketch, parts)
    own, rest = sum_over_rows(mine, other)
    return last_level(core, own, rest, parts)


def solution(mesh):
    split = Mesh(mesh.devices.reshape(8, 4, 4, 2), ROWS)
    return jax.shard_map(
        per_device,
        mesh=split,
        in_specs=(P(ROWS, None), P(None, ROWS), P(), P()),
        out_specs=P(ROWS, None),
        check_vma=False,
    )
```

```python
import jax
import jax.numpy as jnp
from jax import lax
from jax.experimental import pallas as pl
from jax.experimental.pallas import tpu as pltpu
from jax.sharding import Mesh
from jax.sharding import PartitionSpec as P

HALF = 64
ROWS = ("z", "y", "x", "c")
F32 = jnp.float32
BF16 = jnp.bfloat16
BLOCK = 128
PANEL = 16
VMEM = pl.BlockSpec(memory_space=pltpu.VMEM)
SMEM = pl.BlockSpec(memory_space=pltpu.SMEM)
HBM = pl.BlockSpec(memory_space=pltpu.HBM)
PARAMS = pltpu.CompilerParams(vmem_limit_bytes=40 * 2**20)


def split2(x):
    h = x.astype(BF16)
    return h, (x - h.astype(F32)).astype(BF16)


def split3(x):
    h = x.astype(BF16)
    r = x - h.astype(F32)
    m = r.astype(BF16)
    return h, m, (r - m.astype(F32)).astype(BF16)


def mul(a, b, dims=(1, 0)):
    return lax.dot_general(a, b, (((dims[0],), (dims[1],)), ((), ())), preferred_element_type=F32)


def near_dot(a, b, dims=(1, 0)):
    return mul(a[0], b[0], dims) + (mul(a[0], b[1], dims) + mul(a[1], b[0], dims))


def exact_dot(a, b):
    ah, am, al = split3(a)
    bh, bm, bl = split3(b)
    hm = jnp.concatenate([ah, am], 1)
    low = mul(hm, jnp.concatenate([bm, bm], 0))
    low += mul(jnp.concatenate([al, ah], 1), jnp.concatenate([bh, bl], 0))
    return mul(hm, jnp.concatenate([bh, bh], 0)) + low


def factor_block(d_block):
    n = d_block.shape[0]
    count = n // PANEL
    rows = [d_block[i : i + 8] for i in range(0, n, 8)]
    sub = lax.broadcasted_iota(jnp.int32, (8, n), 0)
    lane = lax.broadcasted_iota(jnp.int32, (8, n), 1)
    spread = lambda x, r: jnp.broadcast_to(x[r % 8 : r % 8 + 1], (8, n))
    lanes = lambda x, at: jnp.broadcast_to(x[:, at : at + 1], (8, n))
    both = range(2)
    inverse = []
    for p in range(count):
        at = PANEL * p
        ours = (lane >= at) & (lane < at + PANEL)
        a = rows[2 * p : 2 * p + 2]
        cols = [[lanes(a[h], at + j) for h in both] for j in range(PANEL)]
        if p + 1 < count:
            below = [[lanes(rows[2 * p + 2 + h], at + j) for h in both] for j in range(PANEL)]
        left = rows[2 * p + 4 :]
        a = [jnp.where(ours, (lane == sub + (at + 8 * h)).astype(F32), a[h]) for h in both]
        w = [jnp.zeros((8, n), F32)] * 2
        scale = [jnp.zeros((8, n), F32)] * 2
        d = spread(cols[0][0], 0)
        for k in range(PANEL):
            g = k // 8
            here = sub == k % 8
            root = lax.rsqrt(d)
            inv = root * root
            m = list(cols[k])
            if k + 1 < PANEL:
                e = (k + 1) // 8
                cross = spread(m[e], k + 1) * spread(cols[k + 1][g], k)
                d = spread(cols[k + 1][e], k + 1) - cross * inv
            m[g] = jnp.where(here, 0.0, m[g])
            m = [m[h] * inv for h in both]
            row = spread(a[g], k)
            w[g] = jnp.where(here, row * root, w[g])
            scale[g] = jnp.where(here, inv, scale[g])
            a = [a[h] - m[h] * row for h in both]
            for j in range(k + 1, PANEL):
                c = spread(cols[j][g], k)
                cols[j] = [cols[j][h] - m[h] * c for h in both]
        inverse += w
        if p + 1 < count:
            a = [a[h] * scale[h] for h in both]
            wide = [spread(a[j // 8], j) for j in range(PANEL)]
            for h in both:
                r = 2 * p + 2 + h
                terms = [below[j][h] * wide[j] for j in range(PANEL)]
                while len(terms) > 1:
                    terms = [x + y for x, y in zip(terms[::2], terms[1::2])]
                rows[r] = jnp.where(ours, 0.0, rows[r]) - terms[0]
        if p + 2 < count:
            parts = ([jnp.zeros((at, n), F32)] if p else []) + a + [jnp.zeros((n - at - PANEL, n), F32)]
            change = exact_dot(jnp.concatenate(left, 0), jnp.concatenate(parts, 0))
            for i, r in enumerate(range(2 * p + 4, n // 8)):
                rows[r] = jnp.where(ours, 0.0, rows[r]) - change[8 * i : 8 * i + 8]
    inverse = jnp.concatenate(inverse, 0)
    row_ids = lax.broadcasted_iota(jnp.int32, (n, n), 0)
    return jnp.where(lax.broadcasted_iota(jnp.int32, (n, n), 1) <= row_ids, inverse, 0.0)


def invert_factor(work_ref, row_ref, inv_ref, beside):
    n = BLOCK
    count = work_ref.shape[0] // n
    lane = lax.broadcasted_iota(jnp.int32, (n, count * n), 1) // n

    def step(b, carry):
        at = pl.multiple_of(b * n, n)
        d_block = work_ref[pl.ds(at, n), pl.ds(at, n)]
        beside(b, at)
        w = factor_block(d_block)
        row = exact_dot(w, work_ref[pl.ds(at, n), :])
        row = jnp.where(lane == b, jnp.concatenate([w] * count, 1), row)
        row_ref[...] = row
        high, low = split2(jnp.where(lane <= b, row, 0.0))
        inv_ref[0, pl.ds(at, n), :] = high
        inv_ref[1, pl.ds(at, n), :] = low

        def trail(i, carry):
            to = pl.multiple_of(i * n, n)
            left = row_ref[:, pl.ds(to, n)].T
            kept = jnp.where(lane == b, 0.0, work_ref[pl.ds(to, n), :])
            work_ref[pl.ds(to, n), :] = kept - exact_dot(left, row_ref[...])
            return carry

        lax.fori_loop(b + 1, count, trail, 0)
        return carry

    lax.fori_loop(0, count, step, 0)


def normal_matrix(own, rest, work_ref):
    size = work_ref.shape[0]
    parts = [split3(own), split3(rest)]
    for at in range(0, size, BLOCK):
        total = jnp.zeros((BLOCK, size - at), F32)
        for i, j in ((1, 1), (2, 0), (0, 2), (1, 0), (0, 1), (0, 0)):
            for side in parts:
                total += mul(side[i][:, at : at + BLOCK], side[j][:, at:], (0, 0))
        if at:
            work_ref[at : at + BLOCK, :at] = jnp.zeros((BLOCK, at), F32)
        work_ref[at : at + BLOCK, at:] = total


def copies(pairs, sems):
    return [pltpu.make_async_copy(src, dst, sems.at[i]) for i, (src, dst) in enumerate(pairs)]


def pack_body(core, mid, v_mid, near, far, sems):
    c = core[0]
    edge = 2 * HALF
    reach = 3 * HALF
    moves = []
    for out, high in ((near, 1 - c), (far, c)):
        at = pl.multiple_of(high * (mid.shape[0] - reach), HALF)
        count = mid.shape[1] // edge
        for i in range(count):
            src = mid.at[pl.ds(at, reach), pl.ds(i * edge, edge)]
            moves.append((src, out.at[pl.ds(i * reach, reach)]))
        at = pl.multiple_of(high * (v_mid.shape[1] - edge), edge)
        moves.append((v_mid.at[:, pl.ds(at, edge)], out.at[pl.ds(count * reach, v_mid.shape[0])]))
    moves = copies(moves, sems)
    for move in moves:
        move.start()
    for move in moves:
        move.wait()


def powers_body(
    core, off, near, far, mid_hbm, v_hbm, sketch_hbm, mine, other, parts_hbm, dense, long_ref, mid, v_mid, sketch, parts, sems
):
    n = BLOCK
    size = mid.shape[0]
    width = mid.shape[1]
    reach = 3 * HALF
    blocks = size // n + 2
    c = core[0]
    fetch = copies(((v_hbm, v_mid), (mid_hbm, mid), (sketch_hbm, sketch)), sems)
    for move in fetch:
        move.start()
    sides = ((near, 1 - c), (far, c))
    sub = lax.broadcasted_iota(jnp.int32, (8, 2 * n), 0)
    lanes = lax.broadcasted_iota(jnp.int32, (8, 2 * n), 1)
    hot = []
    for g in range(0, off.shape[0], 8):
        at = jnp.zeros((8, 2 * n), jnp.int32)
        for r in range(8):
            at = jnp.where(sub == r, off[g + r], at)
        hot.append((at + HALF == lanes).astype(F32))
    hot = jnp.concatenate(hot, 0).astype(BF16)
    hot = jnp.concatenate([hot, hot], 0)

    def spread(v, i):
        block = mul(jnp.concatenate(split2(v), 0), hot, (0, 0))
        block = pltpu.roll(block, 0, 1, stride=1, stride_axis=0)
        dense[0, i], dense[1, i] = split2(block)

    for side, below in sides:
        at = pl.multiple_of(below * (reach + size), HALF)
        for i in range(width // n):
            for half, b in enumerate(split2(side[reach * i : reach * (i + 1)])):
                long_ref[half, 0, pl.ds(at, reach), n * i : n * (i + 1)] = b
        spread(side[reach * (width // n) :], below * (blocks - 1))
    fetch[0].wait()
    for i in range(1, blocks - 1):
        spread(v_mid[:, n * (i - 1) : n * i], i)
    fetch[1].wait()
    for half, b in enumerate(split2(mid[...])):
        long_ref[half, 0, reach : reach + size] = b
        parts[half, 0] = b
        edge = jnp.zeros((HALF, width), BF16)
        for level in (1, 2):
            long_ref[half, level, :HALF] = edge
            long_ref[half, level, size + 2 * reach - HALF :] = edge
    store = copies([(parts.at[:, level], parts_hbm.at[:, level]) for level in range(4)], sems.at[pl.ds(3, 4)])
    store[0].start()
    for level in range(3):
        for i in range(blocks) if level < 2 else range(1, blocks - 1):
            window = [long_ref[half, level, n * i : n * i + 2 * n] for half in range(2)]
            result = split2(near_dot((dense[0, i], dense[1, i]), window))
            for half in range(2):
                if level < 2:
                    long_ref[half, level + 1, n * i + HALF : n * i + HALF + n] = result[half]
                if 0 < i < blocks - 1:
                    parts[half, level + 1, n * (i - 1) : n * i] = result[half]
        store[level + 1].start()
    fetch[2].wait()
    gram_halves(core, parts, sketch, mine, other)
    for move in store:
        move.wait()


def gram_halves(core, parts, sketch, mine, other):
    size = parts.shape[2]
    top, low = (split2(sketch[size * s : size * (s + 1)]) for s in range(2))
    get = lambda s: (parts[0, s], parts[1, s])
    projected = split2(near_dot(get(0), top) + near_dot(get(1), low))
    c = core[0]
    mine[...] = near_dot(get(c), projected, (0, 0))
    other[...] = near_dot(get(1 - c), projected, (0, 0))


def basis_products(core, own, rest, parts, work, row, inv, halves, reached, arrived):
    c = core[0]
    normal_matrix(own[...], rest[...], work)
    halves[0, 0], halves[1, 0] = split2(own[...])
    halves[0, 1], halves[1, 1] = split2(rest[...])

    def beside(b, at):
        arrived(b)
        get = lambda s: (parts[0, s, pl.ds(at, BLOCK)], parts[1, s, pl.ds(at, BLOCK)])
        for s in range(reached.shape[1]):
            total = near_dot(get(2 * s + c), (halves[0, 0], halves[1, 0]))
            total += near_dot(get(2 * s + 1 - c), (halves[0, 1], halves[1, 1]))
            reached[0, s, pl.ds(at, BLOCK)], reached[1, s, pl.ds(at, BLOCK)] = split2(total)

    invert_factor(work, row, inv, beside)


def share(src, dst, sems, b):
    rows = pl.ds(pl.multiple_of(b * BLOCK, BLOCK), BLOCK)
    return pltpu.make_async_copy(src.at[:, :, rows], dst.at[:, :, rows], sems.at[b])


def next_body(
    core, own, rest, sketch_hbm, parts_hbm, mine, other, new_hbm, work, row, inv, halves, reached, parts, sketch, new_parts, sems
):
    blocks = parts.shape[2] // BLOCK
    for b in range(blocks):
        share(parts_hbm, parts, sems, b).start()
    fetch, store = copies(((sketch_hbm, sketch), (new_parts, new_hbm)), sems.at[pl.ds(blocks, 2)])
    fetch.start()
    arrived = lambda b: share(parts_hbm, parts, sems, b).wait()
    basis_products(core, own, rest, parts, work, row, inv, halves, reached, arrived)
    for s in range(2):
        result = near_dot((reached[0, s], reached[1, s]), (inv[0], inv[1]), (1, 1))
        new_parts[0, s], new_parts[1, s] = split2(result)
    store.start()
    fetch.wait()
    gram_halves(core, new_parts, sketch, mine, other)
    store.wait()


def last_body(core, own, rest, parts_hbm, out, work, row, inv, halves, reached, parts, sems):
    for b in range(parts.shape[2] // BLOCK):
        share(parts_hbm, parts, sems, b).start()
    arrived = lambda b: share(parts_hbm, parts, sems, b).wait()
    basis_products(core, own, rest, parts, work, row, inv, halves, reached, arrived)
    out[...] = near_dot((reached[0, 0], reached[1, 0]), (inv[0], inv[1]), (1, 1))


def shaped(*shape, dtype=F32):
    return jax.ShapeDtypeStruct(shape, dtype)


def inverse_scratch(size, width, count):
    return [
        pltpu.VMEM((width, width), F32),
        pltpu.VMEM((BLOCK, width), F32),
        pltpu.VMEM((2, width, width), BF16),
        pltpu.VMEM((2, 2, width, width), BF16),
        pltpu.VMEM((2, count, size, width), BF16),
        pltpu.VMEM((2, 2 * count, size, width), BF16),
    ]


def pack(core, mid, v_mid):
    shape = shaped(3 * HALF * mid.shape[1] // BLOCK + v_mid.shape[0], BLOCK)
    return pl.pallas_call(
        pack_body,
        out_shape=(shape, shape),
        in_specs=[SMEM, HBM, HBM],
        out_specs=(VMEM, VMEM),
        scratch_shapes=[pltpu.SemaphoreType.DMA((2 * (mid.shape[1] // BLOCK + 1),))],
        compiler_params=PARAMS,
        name="pack",
    )(core, mid, v_mid)


def powers(core, off, near, far, mid, v_mid, sketch):
    size, width = mid.shape
    return pl.pallas_call(
        powers_body,
        out_shape=(shaped(width, width), shaped(width, width), pltpu.HBM((2, 4, size, width), BF16)),
        in_specs=[SMEM] * 2 + [VMEM] * 2 + [HBM] * 3,
        out_specs=(VMEM, VMEM, HBM),
        scratch_shapes=[
            pltpu.VMEM((2, size // BLOCK + 2, BLOCK, 2 * BLOCK), BF16),
            pltpu.VMEM((2, 3, size + 6 * HALF, width), BF16),
            pltpu.VMEM(mid.shape, F32),
            pltpu.VMEM(v_mid.shape, F32),
            pltpu.VMEM(sketch.shape, F32),
            pltpu.VMEM((2, 4, size, width), BF16),
            pltpu.SemaphoreType.DMA((7,)),
        ],
        compiler_params=PARAMS,
        name="powers",
    )(core, off, near, far, mid, v_mid, sketch)


def next_level(core, own, rest, sketch, parts):
    size, width = parts.shape[2:]
    return pl.pallas_call(
        next_body,
        out_shape=(shaped(width, width), shaped(width, width), pltpu.HBM((2, 2, size, width), BF16)),
        in_specs=[SMEM] + [VMEM] * 2 + [HBM] * 2,
        out_specs=(VMEM, VMEM, HBM),
        scratch_shapes=inverse_scratch(size, width, 2)
        + [
            pltpu.VMEM(sketch.shape, F32),
            pltpu.VMEM((2, 2, size, width), BF16),
            pltpu.SemaphoreType.DMA((size // BLOCK + 2,)),
        ],
        compiler_params=PARAMS,
        name="next_level",
    )(core, own, rest, sketch, parts)


def last_level(core, own, rest, parts):
    size, width = parts.shape[2:]
    return pl.pallas_call(
        last_body,
        out_shape=shaped(size, width),
        in_specs=[SMEM] + [VMEM] * 2 + [HBM],
        out_specs=VMEM,
        scratch_shapes=inverse_scratch(size, width, 1) + [pltpu.SemaphoreType.DMA((size // BLOCK,))],
        compiler_params=PARAMS,
        name="last_level",
    )(core, own, rest, parts)


def swap_cores(x):
    return lax.ppermute(x, "c", [(0, 1), (1, 0)])


def sum_over_rows(mine, other):
    half = mine + swap_cores(other)
    plane = lax.axis_size("y") * lax.axis_size("x")
    rows, width = half.shape
    blocks = half.reshape(plane, rows // plane, width)
    part = lax.all_to_all(blocks, ("y", "x"), 0, 0, tiled=True).sum(0)
    size = lax.axis_size("z")
    for pairs in (
        [(i, i ^ 1) for i in range(size)],
        [(i, i ^ 2) for i in range(size)],
        [(i, size - 1 - i) for i in range(size)],
    ):
        part = part + lax.ppermute(part, "z", pairs)
    copies = jnp.broadcast_to(part[None], blocks.shape)
    own = lax.all_to_all(copies, ("y", "x"), 0, 0, tiled=True).reshape(rows, width)
    return own, swap_cores(own)


def swap_chips(x):
    size = lax.axis_size(ROWS)
    pairs = [(i, i + 1) for i in range(1, size - 1, 2)]
    return lax.ppermute(x, ROWS, pairs + [(j, i) for i, j in pairs])


def per_device(factor_b, band_vals, offsets, sketch):
    core = lax.axis_index("c").reshape(1)
    factor_b, band_vals, sketch = (pltpu.with_memory_space_constraint(x, pltpu.HBM) for x in (factor_b, band_vals, sketch))
    near, far = pack(core, factor_b, band_vals)
    near, far = swap_cores(near), swap_chips(far)
    mine, other, parts = powers(core, offsets, near, far, factor_b, band_vals, sketch)
    own, rest = sum_over_rows(mine, other)
    parts = pltpu.with_memory_space_constraint(parts, pltpu.HBM)
    mine, other, parts = next_level(core, own, rest, sketch, parts)
    own, rest = sum_over_rows(mine, other)
    parts = pltpu.with_memory_space_constraint(parts, pltpu.HBM)
    return last_level(core, own, rest, parts)


def solution(mesh):
    split = Mesh(mesh.devices.reshape(8, 4, 4, 2), ROWS)
    return jax.shard_map(
        per_device,
        mesh=split,
        in_specs=(P(ROWS, None), P(None, ROWS), P(), P()),
        out_specs=P(ROWS, None),
        check_vma=False,
    )
```

```python
import jax
import jax.numpy as jnp
from jax import lax
from jax.experimental import pallas as pl
from jax.experimental.pallas import tpu as pltpu
from jax.sharding import Mesh
from jax.sharding import PartitionSpec as P

HALF = 64
ROWS = ("z", "y", "x", "c")
F32 = jnp.float32
BF16 = jnp.bfloat16
BLOCK = 128
PANEL = 16
VMEM = pl.BlockSpec(memory_space=pltpu.VMEM)
SMEM = pl.BlockSpec(memory_space=pltpu.SMEM)
HBM = pl.BlockSpec(memory_space=pltpu.HBM)
PARAMS = pltpu.CompilerParams(vmem_limit_bytes=40 * 2**20)


def split2(x):
    h = x.astype(BF16)
    return h, (x - h.astype(F32)).astype(BF16)


def split3(x):
    h = x.astype(BF16)
    r = x - h.astype(F32)
    m = r.astype(BF16)
    return h, m, (r - m.astype(F32)).astype(BF16)


def mul(a, b, dims=(1, 0)):
    return lax.dot_general(a, b, (((dims[0],), (dims[1],)), ((), ())), preferred_element_type=F32)


def near_dot(a, b, dims=(1, 0)):
    return mul(a[0], b[0], dims) + (mul(a[0], b[1], dims) + mul(a[1], b[0], dims))


def exact_dot(a, b):
    ah, am, al = split3(a)
    bh, bm, bl = split3(b)
    hm = jnp.concatenate([ah, am], 1)
    low = mul(hm, jnp.concatenate([bm, bm], 0))
    low += mul(jnp.concatenate([al, ah], 1), jnp.concatenate([bh, bl], 0))
    return mul(hm, jnp.concatenate([bh, bh], 0)) + low


def factor_block(d_block):
    n = d_block.shape[0]
    count = n // PANEL
    rows = [d_block[i : i + 8] for i in range(0, n, 8)]
    sub = lax.broadcasted_iota(jnp.int32, (8, n), 0)
    lane = lax.broadcasted_iota(jnp.int32, (8, n), 1)
    spread = lambda x, r: jnp.broadcast_to(x[r % 8 : r % 8 + 1], (8, n))
    lanes = lambda x, at: jnp.broadcast_to(x[:, at : at + 1], (8, n))
    both = range(2)
    inverse = []
    for p in range(count):
        at = PANEL * p
        ours = (lane >= at) & (lane < at + PANEL)
        a = rows[2 * p : 2 * p + 2]
        cols = [[lanes(a[h], at + j) for h in both] for j in range(PANEL)]
        if p + 1 < count:
            below = [[lanes(rows[2 * p + 2 + h], at + j) for h in both] for j in range(PANEL)]
        left = rows[2 * p + 4 :]
        a = [jnp.where(ours, (lane == sub + (at + 8 * h)).astype(F32), a[h]) for h in both]
        w = [jnp.zeros((8, n), F32)] * 2
        scale = [jnp.zeros((8, n), F32)] * 2
        d = spread(cols[0][0], 0)
        for k in range(PANEL):
            g = k // 8
            here = sub == k % 8
            root = lax.rsqrt(d)
            inv = root * root
            m = list(cols[k])
            if k + 1 < PANEL:
                e = (k + 1) // 8
                cross = spread(m[e], k + 1) * spread(cols[k + 1][g], k)
                d = spread(cols[k + 1][e], k + 1) - cross * inv
            m[g] = jnp.where(here, 0.0, m[g])
            m = [m[h] * inv for h in both]
            row = spread(a[g], k)
            w[g] = jnp.where(here, row * root, w[g])
            scale[g] = jnp.where(here, inv, scale[g])
            a = [a[h] - m[h] * row for h in both]
            for j in range(k + 1, PANEL):
                c = spread(cols[j][g], k)
                cols[j] = [cols[j][h] - m[h] * c for h in both]
        inverse += w
        if p + 1 < count:
            a = [a[h] * scale[h] for h in both]
            wide = [spread(a[j // 8], j) for j in range(PANEL)]
            for h in both:
                r = 2 * p + 2 + h
                terms = [below[j][h] * wide[j] for j in range(PANEL)]
                while len(terms) > 1:
                    terms = [x + y for x, y in zip(terms[::2], terms[1::2])]
                rows[r] = jnp.where(ours, 0.0, rows[r]) - terms[0]
        if p + 2 < count:
            parts = ([jnp.zeros((at, n), F32)] if p else []) + a + [jnp.zeros((n - at - PANEL, n), F32)]
            change = exact_dot(jnp.concatenate(left, 0), jnp.concatenate(parts, 0))
            for i, r in enumerate(range(2 * p + 4, n // 8)):
                rows[r] = jnp.where(ours, 0.0, rows[r]) - change[8 * i : 8 * i + 8]
    inverse = jnp.concatenate(inverse, 0)
    row_ids = lax.broadcasted_iota(jnp.int32, (n, n), 0)
    return jnp.where(lax.broadcasted_iota(jnp.int32, (n, n), 1) <= row_ids, inverse, 0.0)


def invert_factor(work_ref, row_ref, inv_ref, beside):
    n = BLOCK
    count = work_ref.shape[0] // n
    lane = lax.broadcasted_iota(jnp.int32, (n, count * n), 1) // n

    def step(b, carry):
        at = pl.multiple_of(b * n, n)
        d_block = work_ref[pl.ds(at, n), pl.ds(at, n)]
        beside(b, at)
        w = factor_block(d_block)
        row = exact_dot(w, work_ref[pl.ds(at, n), :])
        row = jnp.where(lane == b, jnp.concatenate([w] * count, 1), row)
        row_ref[...] = row
        high, low = split2(jnp.where(lane <= b, row, 0.0))
        inv_ref[0, pl.ds(at, n), :] = high
        inv_ref[1, pl.ds(at, n), :] = low

        def trail(i, carry):
            to = pl.multiple_of(i * n, n)
            left = row_ref[:, pl.ds(to, n)].T
            kept = jnp.where(lane == b, 0.0, work_ref[pl.ds(to, n), :])
            work_ref[pl.ds(to, n), :] = kept - exact_dot(left, row_ref[...])
            return carry

        lax.fori_loop(b + 1, count, trail, 0)
        return carry

    lax.fori_loop(0, count, step, 0)


def add_normal(side, into, onto=None):
    size = into.shape[0]
    parts = split3(side)
    for at in range(0, size, BLOCK):
        total = jnp.zeros((BLOCK, size - at), F32)
        for i, j in ((1, 1), (2, 0), (0, 2), (1, 0), (0, 1), (0, 0)):
            total += mul(parts[i][:, at : at + BLOCK], parts[j][:, at:], (0, 0))
        if onto is not None:
            total += onto[at : at + BLOCK, at:]
        if at:
            into[at : at + BLOCK, :at] = jnp.zeros((BLOCK, at), F32)
        into[at : at + BLOCK, at:] = total


def copies(pairs, sems):
    return [pltpu.make_async_copy(src, dst, sems.at[i]) for i, (src, dst) in enumerate(pairs)]


def pack_body(core, mid, v_mid, near, far, sems):
    c = core[0]
    edge = 2 * HALF
    reach = 3 * HALF
    moves = []
    for out, high in ((near, 1 - c), (far, c)):
        at = pl.multiple_of(high * (mid.shape[0] - reach), HALF)
        count = mid.shape[1] // edge
        for i in range(count):
            src = mid.at[pl.ds(at, reach), pl.ds(i * edge, edge)]
            moves.append((src, out.at[pl.ds(i * reach, reach)]))
        at = pl.multiple_of(high * (v_mid.shape[1] - edge), edge)
        moves.append((v_mid.at[:, pl.ds(at, edge)], out.at[pl.ds(count * reach, v_mid.shape[0])]))
    moves = copies(moves, sems)
    for move in moves:
        move.start()
    for move in moves:
        move.wait()


def spread_bands(v, hot, dense, i):
    block = mul(jnp.concatenate(split2(v), 0), hot, (0, 0))
    dense[0, i], dense[1, i] = split2(pltpu.roll(block, 0, 1, stride=1, stride_axis=0))


def ready_body(off, v_hbm, mid_hbm, sketch_hbm, hot_ref, dense, parts, projected, mid, v_mid, sketch, sems):
    n = BLOCK
    fetch = copies(((v_hbm, v_mid), (mid_hbm, mid), (sketch_hbm.at[pl.ds(0, mid.shape[0])], sketch)), sems)
    for move in fetch:
        move.start()
    sub = lax.broadcasted_iota(jnp.int32, (8, 2 * n), 0)
    lanes = lax.broadcasted_iota(jnp.int32, (8, 2 * n), 1)
    hot = []
    for g in range(0, off.shape[0], 8):
        at = jnp.zeros((8, 2 * n), jnp.int32)
        for r in range(8):
            at = jnp.where(sub == r, off[g + r], at)
        hot.append((at + HALF == lanes).astype(F32))
    hot = jnp.concatenate(hot, 0).astype(BF16)
    hot = jnp.concatenate([hot, hot], 0)
    hot_ref[...] = hot
    fetch[0].wait()
    for i in range(dense.shape[1]):
        spread_bands(v_mid[:, n * i : n * (i + 1)], hot, dense, i)
    fetch[1].wait()
    parts[0], parts[1] = split2(mid[...])
    fetch[2].wait()
    projected[...] = near_dot((parts[0], parts[1]), split2(sketch[...]))


def apply_bands(dense, source, i, n):
    window = [source[half, n * i : n * i + 2 * n] for half in range(2)]
    return split2(near_dot((dense[0], dense[1]), window))


def first_body(
    core, near, far, hot, dense, mid, half_projected, sketch_hbm, mine, other, parts_hbm, power, dense_rim, long_ref, sketch, parts, sems
):
    n = BLOCK
    size, width = mid.shape[1:]
    reach = 3 * HALF
    inner = size // n
    c = core[0]
    fetch, keep, store = copies(
        ((sketch_hbm.at[pl.ds(size, size)], sketch), (mid, parts_hbm.at[:, 0]), (parts, parts_hbm.at[:, 1])), sems
    )
    fetch.start()
    keep.start()
    long_ref[:, reach : reach + size] = mid[...]
    edge = jnp.zeros((2, HALF, width), BF16)
    power[:, :HALF] = edge
    power[:, size + 2 * reach - HALF :] = edge
    for side, below in ((near, 1 - c), (far, c)):
        at = pl.multiple_of(below * (reach + size), HALF)
        for i in range(width // n):
            for half, b in enumerate(split2(side[reach * i : reach * (i + 1)])):
                long_ref[half, pl.ds(at, reach), n * i : n * (i + 1)] = b
        spread_bands(side[reach * (width // n) :], hot[...], dense_rim, below)
    for i in range(inner + 2):
        if 0 < i <= inner:
            block = (dense[0, i - 1], dense[1, i - 1])
        else:
            block = (dense_rim[0, i // (inner + 1)], dense_rim[1, i // (inner + 1)])
        for half, b in enumerate(apply_bands(block, long_ref, i, n)):
            power[half, n * i + HALF : n * i + HALF + n] = b
            if 0 < i <= inner:
                parts[half, n * (i - 1) : n * i] = b
    store.start()
    fetch.wait()
    projected = split2(half_projected[...] + near_dot((parts[0], parts[1]), split2(sketch[...])))
    keep.wait()

    def gram(first):
        picked = [jnp.where(first, mid[half], parts[half]) for half in range(2)]
        return near_dot(picked, projected, (0, 0))

    mine[...] = gram(c == 0)
    other[...] = gram(c == 1)
    store.wait()


def higher_body(power, dense, dense_rim, parts_hbm, long_ref, parts, sems):
    n = BLOCK
    size = parts.shape[2]
    inner = size // n
    for level in range(2):
        source = long_ref if level else power
        for i in range(level, inner + 2 - level):
            if 0 < i <= inner:
                block = (dense[0, i - 1], dense[1, i - 1])
            else:
                block = (dense_rim[0, i // (inner + 1)], dense_rim[1, i // (inner + 1)])
            for half, b in enumerate(apply_bands(block, source, i, n)):
                if level == 0:
                    long_ref[half, n * i + HALF : n * i + HALF + n] = b
                if 0 < i <= inner:
                    parts[half, level, n * (i - 1) : n * i] = b
    store = copies(((parts, parts_hbm),), sems)[0]
    store.start()
    store.wait()


def gram_halves(core, parts, sketch, mine, other):
    size = parts.shape[2]
    top, low = (split2(sketch[size * s : size * (s + 1)]) for s in range(2))
    get = lambda s: (parts[0, s], parts[1, s])
    projected = split2(near_dot(get(0), top) + near_dot(get(1), low))
    c = core[0]
    mine[...] = near_dot(get(c), projected, (0, 0))
    other[...] = near_dot(get(1 - c), projected, (0, 0))


def own_body(core, own, *rest):
    count = len(rest) - 4
    sources, (normal, reached, parts, sems) = rest[:count], rest[count:]
    fetch = copies([(src.at[:, core[0]], parts.at[:, s]) for s, src in enumerate(sources)], sems)
    for move in fetch:
        move.start()
    add_normal(own[...], normal)
    side = split2(own[...])
    for s in range(count):
        fetch[s].wait()
        reached[s] = near_dot((parts[0, s], parts[1, s]), side)


def basis_products(core, rest, normal, reached_own, sources, work, row, inv, halves, reached, parts, sems):
    fetch = copies([(src.at[:, 1 - core[0]], parts.at[:, s]) for s, src in enumerate(sources)], sems)
    for move in fetch:
        move.start()
    add_normal(rest[...], work, normal)
    halves[0], halves[1] = split2(rest[...])
    for move in fetch:
        move.wait()

    def beside(b, at):
        rows = pl.ds(at, BLOCK)
        for s in range(len(sources)):
            total = reached_own[s, rows] + near_dot((parts[0, s, rows], parts[1, s, rows]), (halves[0], halves[1]))
            reached[0, s, rows], reached[1, s, rows] = split2(total)

    invert_factor(work, row, inv, beside)


def next_body(
    core, rest, normal, reached_own, sketch_hbm, low_hbm, high_hbm, mine, other, new_hbm, work, row, inv, halves, reached, parts, sems, sketch, new_parts
):
    fetch, store = copies(((sketch_hbm, sketch), (new_parts, new_hbm)), sems.at[pl.ds(2, 2)])
    fetch.start()
    basis_products(core, rest, normal, reached_own, (low_hbm, high_hbm), work, row, inv, halves, reached, parts, sems)
    for s in range(2):
        result = near_dot((reached[0, s], reached[1, s]), (inv[0], inv[1]), (1, 1))
        new_parts[0, s], new_parts[1, s] = split2(result)
    store.start()
    fetch.wait()
    gram_halves(core, new_parts, sketch, mine, other)
    store.wait()


def last_body(core, rest, normal, reached_own, parts_hbm, out, work, row, inv, halves, reached, parts, sems):
    basis_products(core, rest, normal, reached_own, (parts_hbm,), work, row, inv, halves, reached, parts, sems)
    out[...] = near_dot((reached[0, 0], reached[1, 0]), (inv[0], inv[1]), (1, 1))


def shaped(*shape, dtype=F32):
    return jax.ShapeDtypeStruct(shape, dtype)


def inverse_scratch(size, width, count):
    return [
        pltpu.VMEM((width, width), F32),
        pltpu.VMEM((BLOCK, width), F32),
        pltpu.VMEM((2, width, width), BF16),
        pltpu.VMEM((2, width, width), BF16),
        pltpu.VMEM((2, count, size, width), BF16),
        pltpu.VMEM((2, count, size, width), BF16),
        pltpu.SemaphoreType.DMA((4,)),
    ]


def pack(core, mid, v_mid):
    shape = shaped(3 * HALF * mid.shape[1] // BLOCK + v_mid.shape[0], BLOCK)
    return pl.pallas_call(
        pack_body,
        out_shape=(shape, shape),
        in_specs=[SMEM, HBM, HBM],
        out_specs=(VMEM, VMEM),
        scratch_shapes=[pltpu.SemaphoreType.DMA((2 * (mid.shape[1] // BLOCK + 1),))],
        compiler_params=PARAMS,
        name="pack",
    )(core, mid, v_mid)


def kernel(body, name, args, specs, out, out_specs, scratch):
    return pl.pallas_call(
        body,
        out_shape=out,
        in_specs=specs,
        out_specs=out_specs,
        scratch_shapes=scratch,
        compiler_params=PARAMS,
        name=name,
    )(*args)


def ready(off, mid, v_mid, sketch):
    size, width = mid.shape
    out = (
        shaped(2 * v_mid.shape[0], 2 * BLOCK, dtype=BF16),
        shaped(2, size // BLOCK, BLOCK, 2 * BLOCK, dtype=BF16),
        shaped(2, size, width, dtype=BF16),
        shaped(size, width),
    )
    scratch = [pltpu.VMEM(x.shape, F32) for x in (mid, v_mid, mid)] + [pltpu.SemaphoreType.DMA((3,))]
    return kernel(ready_body, "ready", (off, v_mid, mid, sketch), [SMEM] + [HBM] * 3, out, (VMEM,) * 4, scratch)


def first(core, near, far, hot, dense, mid, projected, sketch):
    size, width = projected.shape
    out = (
        shaped(width, width),
        shaped(width, width),
        pltpu.HBM((2, 2, size, width), BF16),
        shaped(2, size + 6 * HALF, width, dtype=BF16),
        shaped(2, 2, BLOCK, 2 * BLOCK, dtype=BF16),
    )
    scratch = [
        pltpu.VMEM((2, size + 6 * HALF, width), BF16),
        pltpu.VMEM((size, width), F32),
        pltpu.VMEM((2, size, width), BF16),
        pltpu.SemaphoreType.DMA((3,)),
    ]
    args = (core, near, far, hot, dense, mid, projected, sketch)
    return kernel(first_body, "first", args, [SMEM] + [VMEM] * 6 + [HBM], out, (VMEM, VMEM, HBM, VMEM, VMEM), scratch)


def higher(power, dense, dense_rim):
    width = power.shape[2]
    size = dense.shape[1] * BLOCK
    scratch = [pltpu.VMEM(power.shape, BF16), pltpu.VMEM((2, 2, size, width), BF16), pltpu.SemaphoreType.DMA((1,))]
    return kernel(
        higher_body, "higher", (power, dense, dense_rim), [VMEM] * 3, pltpu.HBM((2, 2, size, width), BF16), HBM, scratch
    )


def own_share(core, own, *sources):
    size, width = sources[0].shape[2:]
    count = len(sources)
    out = (shaped(width, width), shaped(count, size, width))
    scratch = [pltpu.VMEM((2, count, size, width), BF16), pltpu.SemaphoreType.DMA((count,))]
    return kernel(own_body, "own_share", (core, own, *sources), [SMEM, VMEM] + [HBM] * count, out, (VMEM,) * 2, scratch)


def next_level(core, rest, normal, reached, sketch, low, high):
    size, width = low.shape[2:]
    out = (shaped(width, width), shaped(width, width), pltpu.HBM((2, 2, size, width), BF16))
    scratch = inverse_scratch(size, width, 2) + [pltpu.VMEM(sketch.shape, F32), pltpu.VMEM((2, 2, size, width), BF16)]
    args = (core, rest, normal, reached, sketch, low, high)
    return kernel(next_body, "next_level", args, [SMEM] + [VMEM] * 3 + [HBM] * 3, out, (VMEM, VMEM, HBM), scratch)


def last_level(core, rest, normal, reached, parts):
    size, width = parts.shape[2:]
    args = (core, rest, normal, reached, parts)
    scratch = inverse_scratch(size, width, 1)
    return kernel(last_body, "last_level", args, [SMEM] + [VMEM] * 3 + [HBM], shaped(size, width), VMEM, scratch)


def swap_cores(x):
    return lax.ppermute(x, "c", [(0, 1), (1, 0)])


def sum_over_rows(mine, other):
    half = mine + swap_cores(other)
    plane = lax.axis_size("y") * lax.axis_size("x")
    rows, width = half.shape
    blocks = half.reshape(plane, rows // plane, width)
    part = lax.all_to_all(blocks, ("y", "x"), 0, 0, tiled=True).sum(0)
    size = lax.axis_size("z")
    for pairs in (
        [(i, i ^ 1) for i in range(size)],
        [(i, i ^ 2) for i in range(size)],
        [(i, size - 1 - i) for i in range(size)],
    ):
        part = part + lax.ppermute(part, "z", pairs)
    copies = jnp.broadcast_to(part[None], blocks.shape)
    own = lax.all_to_all(copies, ("y", "x"), 0, 0, tiled=True).reshape(rows, width)
    return own, swap_cores(own)


def swap_chips(x):
    size = lax.axis_size(ROWS)
    pairs = [(i, i + 1) for i in range(1, size - 1, 2)]
    return lax.ppermute(x, ROWS, pairs + [(j, i) for i, j in pairs])


def in_hbm(*arrays):
    return [pltpu.with_memory_space_constraint(x, pltpu.HBM) for x in arrays]


def per_device(factor_b, band_vals, offsets, sketch):
    core = lax.axis_index("c").reshape(1)
    factor_b, band_vals, sketch = in_hbm(factor_b, band_vals, sketch)
    near, far = pack(core, factor_b, band_vals)
    near, far = swap_cores(near), swap_chips(far)
    hot, dense, mid, projected = ready(offsets, factor_b, band_vals, sketch)
    mine, other, low, power, dense_rim = first(core, near, far, hot, dense, mid, projected, sketch)
    mine, high = lax.optimization_barrier((mine, higher(power, dense, dense_rim)))
    low, high = in_hbm(low, high)
    own, rest = sum_over_rows(mine, other)
    normal, reached = own_share(core, own, low, high)
    mine, other, parts = next_level(core, rest, normal, reached, sketch, low, high)
    own, rest = sum_over_rows(mine, other)
    (parts,) = in_hbm(parts)
    normal, reached = own_share(core, own, parts)
    return last_level(core, rest, normal, reached, parts)


def solution(mesh):
    split = Mesh(mesh.devices.reshape(8, 4, 4, 2), ROWS)
    return jax.shard_map(
        per_device,
        mesh=split,
        in_specs=(P(ROWS, None), P(None, ROWS), P(), P()),
        out_specs=P(ROWS, None),
        check_vma=False,
    )
```
